512 devices in a mesh: grp: 8 (over z), dp: 64 (over y, x, core).
Axes of the slice: x: 4, y: 8, z: 8, core: 2. Of those that a mesh axis runs over, the one named last changes fastest.
Arguments:
- start_state: bfloat16 [65536, 512], P(('grp', 'dp')), may hold values from -24 to 24
- w_up: bfloat16 [512, 1024], replicated, may hold values from -0.25 to 0.25
- b_up: float32 [1024], replicated, may hold values from -3 to 3
- w_down: bfloat16 [1024, 512], replicated, may hold values from -0.1875 to 0.1875
- w_spread: bfloat16 [512, 1024], replicated, may hold values from -0.25 to 0.25
- w_scale: bfloat16 [1024, 512], replicated, may hold values from -0.1875 to 0.1875
- b_scale: float32 [512], replicated, may hold values from -4 to 4
- brownian_noise: bfloat16 [3, 65536, 512], P(None, ('grp', 'dp')), may hold values from -5 to 5
- step_mults: int32 [3, 65536], P(None, ('grp', 'dp')), may hold values from 1 to 4
- accept_flags: int32 [3, 65536], P(None, ('grp', 'dp')), may hold values 0 or 1
- cotangent: bfloat16 [65536, 512], P(('grp', 'dp')), may hold values from -6 to 6
Outputs:
- err_norms: float32 [3], replicated
- grad_up: float32 [512, 1024], P('dp')
- grad_down: float32 [512, 1024], P('dp')
The draws below stay inside these ranges and needn't reach their ends.
All inputs are finite; a program needn't handle non-finite values. No bound on the sum of `accept_flags` on one device may be relied on, other than what follows from the above.
Results may differ from the reference program's by a relative error of at most 0.0033.
Values sent between devices are 32-bit elements; how exact they have to be, the bound alone decides.
No kernel may reach another device: no remote copies, remote signals or barrier semaphores. Data moves between devices by JAX's collectives and lax.ppermute only.
A program may use at most 64 MiB of HBM per device.

```python
import jax
import jax.numpy as jnp
from jax import lax

LATENT = 512
HIDDEN_SIZE = 1024
STEPS = 3
SEQ = 65536


def set_ends(result, stream_key, low, largest):
    place = [jax.random.randint(jax.random.fold_in(stream_key, axis), (), 0, length) for axis, length in enumerate(result.shape)]
    widest = result.shape.index(max(result.shape))
    neighbour = place[:widest] + [(place[widest] + 1) % result.shape[widest]] + place[widest + 1:]
    return result.at[tuple(place)].set(low).at[tuple(neighbour)].set(largest)


def strengthened(drawn, key, source, target, parts, factor):
    owner, partner = [(jnp.arange(drawn.shape[dim]) // (drawn.shape[dim] // parts)).reshape([-1 if axis == dim else 1 for axis in range(drawn.ndim)]) for dim in (source, target)]
    chosen = jax.random.permutation(key, parts)[partner]
    strong = (owner == chosen) | (owner == (partner + parts // 2) % parts)
    return jnp.where(strong, factor * drawn, drawn)


def block_scale(rng, extent, split, least, top_value):
    gain = 1.0
    for position, parts in split:
        steps = jax.random.uniform(jax.random.fold_in(jax.random.fold_in(rng, 6), position), (parts,), jnp.float32, least / len(split), top_value / len(split))
        gain = gain * jnp.repeat(jnp.exp(steps), extent[position] // parts).reshape((-1,) + (1,) * (len(extent) - 1 - position))
    return gain


def normal_values(rng, dims, deviation, reach, split=(), held_as=jnp.bfloat16):
    drawn = jax.random.normal(rng, dims, jnp.float32) * deviation
    if len(split) > 0:
        drawn = block_scale(rng, dims, split, -0.22, 0.18) * drawn
    return jnp.clip(drawn, min=-reach, max=reach).astype(held_as)


def heavy_noise(rng, extent, scale, most, cuts, heavy, dtype=jnp.bfloat16):
    array = scale * jax.random.normal(rng, extent, jnp.float32)
    if cuts:
        array = array * block_scale(rng, extent, cuts, -0.22, 0.18)
    return jnp.clip(strengthened(array, jax.random.fold_in(rng, 3), *heavy), -most, most).astype(dtype)


def setup_inputs(seed: int = 0) -> dict:
    key_list = jax.random.split(jax.random.key(seed), 12)
    start_state = heavy_noise(key_list[0], (SEQ, LATENT), 1.0, 24.0, ((0, 512),), (0, 1, 512, 6.0))
    w_up = normal_values(key_list[1], (LATENT, HIDDEN_SIZE), LATENT ** -0.5, 0.25)
    b_up = normal_values(key_list[2], (HIDDEN_SIZE,), 0.5, 3.0, (), jnp.float32)
    w_down = normal_values(key_list[3], (HIDDEN_SIZE, LATENT), HIDDEN_SIZE ** -0.5, 0.1875)
    w_spread = normal_values(key_list[4], (LATENT, HIDDEN_SIZE), LATENT ** -0.5, 0.25)
    w_scale = normal_values(key_list[5], (HIDDEN_SIZE, LATENT), HIDDEN_SIZE ** -0.5, 0.1875)
    b_scale = normal_values(key_list[6], (LATENT,), 1.0, 4.0, (), jnp.float32)
    brownian_noise = normal_values(key_list[7], (STEPS, SEQ, LATENT), 1.0, 5.0, ((1, 512),))
    step_mults = set_ends(jax.random.randint(key_list[8], (STEPS, SEQ), 1, 5), jax.random.fold_in(key_list[8], 1), 1, 4).astype(jnp.int32)
    accept_flags = set_ends((jax.random.randint(key_list[9], (STEPS, SEQ), 0, 4) < 3).astype(jnp.int32), jax.random.fold_in(key_list[9], 1), 0, 1)
    cotangent = normal_values(key_list[10], (SEQ, LATENT), 1.0, 6.0, ((0, 512),))
    return dict(start_state=start_state, w_up=w_up, b_up=b_up, w_down=w_down, w_spread=w_spread, w_scale=w_scale, b_scale=b_scale, brownian_noise=brownian_noise, step_mults=step_mults, accept_flags=accept_flags, cotangent=cotangent)


base_step = 0.05
abs_tol = 0.01
rel_tol = 0.01

def diffuse(current, w_first, w_second, b_second):
    inner = jax.nn.silu(jnp.dot(current.astype(jnp.bfloat16), w_first, preferred_element_type=jnp.float32))
    outer = jnp.dot(inner.astype(jnp.bfloat16), w_second, preferred_element_type=jnp.float32)
    return 0.6 * jax.nn.sigmoid(outer + b_second)

def forward_step(current, w_up, b_up, w_down, w_spread, w_scale, b_scale, noise_now, mult_now, flag_now):
    low_state = current.astype(jnp.bfloat16)
    pre_act = jnp.dot(low_state, w_up, preferred_element_type=jnp.float32) + b_up
    hidden = jax.nn.silu(pre_act).astype(jnp.bfloat16)
    drift_out = jnp.dot(hidden, w_down, preferred_element_type=jnp.float32)
    step_size = mult_now.astype(jnp.float32)[:, None] * base_step
    sqrt_step = jnp.sqrt(step_size)
    brownian = sqrt_step * noise_now.astype(jnp.float32)
    keep_mask = flag_now.astype(jnp.float32)[:, None]

    def update(before):
        spread = diffuse(before, w_spread, w_scale, b_scale)
        shifted = diffuse(before + spread * sqrt_step, w_spread, w_scale, b_scale)
        milstein = (shifted - spread) * (brownian * brownian - step_size) / (2.0 * sqrt_step)
        proposal = before + drift_out * step_size + spread * brownian + milstein
        return (keep_mask * proposal + (1.0 - keep_mask) * before, milstein)
    (advanced, milstein), pull_back = jax.vjp(update, current)
    scaled = milstein / (abs_tol + rel_tol * jnp.abs(current))
    err_part = jnp.sum(scaled * scaled)
    return (advanced, err_part, (low_state, pre_act, hidden, pull_back, step_size, keep_mask))

def backward_step(cot_state, record, w_up, w_down, grad_up, grad_down):
    low_state, pre_act, hidden, pull_back, step_size, keep_mask = record
    cot_drift = (cot_state * keep_mask * step_size).astype(jnp.bfloat16)
    grad_down = grad_down + lax.dot_general(cot_drift, hidden, (((0,), (0,)), ((), ())), preferred_element_type=jnp.float32)
    sigma = jax.nn.sigmoid(pre_act)
    back_pre = lax.dot_general(cot_drift, w_down, (((1,), (1,)), ((), ())), preferred_element_type=jnp.float32)
    cot_pre = (back_pre * sigma * (1.0 + pre_act * (1.0 - sigma))).astype(jnp.bfloat16)
    grad_up = grad_up + lax.dot_general(low_state, cot_pre, (((0,), (0,)), ((), ())), preferred_element_type=jnp.float32)
    through = pull_back((cot_state, jnp.zeros_like(cot_state)))[0]
    cot_state = through + lax.dot_general(cot_pre, w_up, (((1,), (1,)), ((), ())), preferred_element_type=jnp.float32)
    return (cot_state, grad_up, grad_down)

def reference(start_state, w_up, b_up, w_down, w_spread, w_scale, b_scale, brownian_noise, step_mults, accept_flags, cotangent):
    current = start_state.astype(jnp.float32)
    records = []
    err_sums = []
    for step_index in range(STEPS):
        current, err_part, record = forward_step(current, w_up, b_up, w_down, w_spread, w_scale, b_scale, brownian_noise[step_index], step_mults[step_index], accept_flags[step_index])
        records.append(record)
        err_sums.append(err_part)
    err_norms = jnp.sqrt(jnp.stack(err_sums) / (SEQ * LATENT))
    cot_state = cotangent.astype(jnp.float32)
    grad_up = jnp.zeros((LATENT, HIDDEN_SIZE), jnp.float32)
    grad_down = jnp.zeros((LATENT, HIDDEN_SIZE), jnp.float32)
    for step_index in reversed(range(STEPS)):
        cot_state, grad_up, grad_down = backward_step(cot_state, records[step_index], w_up, w_down, grad_up, grad_down)
    return (err_norms, grad_up, grad_down)
```

```python
import jax
import jax.numpy as jnp
from jax import lax
from jax.experimental import pallas as pl
from jax.experimental.pallas import tpu as pltpu
from jax.sharding import Mesh
from jax.sharding import PartitionSpec as P

DP = ("dp_0", "dp_1", "dp_2")
GRP_DP = ("grp", "dp_0", "dp_1", "dp_2")

base_step = 0.05
abs_tol = 0.01
rel_tol = 0.01
F32 = jnp.float32
BF16 = jnp.bfloat16


def mm(a, b):
    return jnp.dot(a, b, preferred_element_type=F32)


def mm_t(a, b):
    return lax.dot_general(a, b, (((1,), (1,)), ((), ())), preferred_element_type=F32)


def t_mm(a, b):
    return lax.dot_general(a, b, (((0,), (0,)), ((), ())), preferred_element_type=F32)


def sigmoid(x):
    return 0.5 * jnp.tanh(0.5 * x) + 0.5


def steps_kernel(
    core_ref,
    start_hbm, w_up_hbm, b_up_ref, w_down_hbm, w_spread_hbm, w_scale_hbm, b_scale_ref,
    noise_hbm, mults_ref, flags_ref, cot_hbm,
    keep_hbm, send_hbm, err_ref,
    start_v, w_up, w_down, w_spread, w_scale, noise_v, cot_v,
    d_pre, d_one, d_two, hid_v, low_v, cpre_v, cdrift_v, d_g, d_gbar, fac_v, dw_v, out_v,
    in_sems, out_sems,
):
    steps, rows, latent = noise_v.shape
    far, near = out_v.shape[1], out_v.shape[2]
    loads = {}
    for slot, (name, src, dst) in enumerate((
        ("start", start_hbm, start_v),
        ("spread", w_spread_hbm, w_spread),
        ("scale", w_scale_hbm, w_scale),
        ("up", w_up_hbm, w_up),
        ("noise", noise_hbm, noise_v),
        ("down", w_down_hbm, w_down),
        ("cot", cot_hbm, cot_v),
    )):
        loads[name] = pltpu.make_async_copy(src, dst, in_sems.at[slot])
        loads[name].start()

    per_row = jnp.concatenate(
        [
            mults_ref[...].astype(F32) * base_step,
            flags_ref[...].astype(F32),
            jnp.zeros((8 - 2 * steps, rows), F32),
        ],
        axis=0,
    )
    columns = jnp.transpose(per_row)
    b_up = b_up_ref[...]
    b_scale = b_scale_ref[...]

    loads["start"].wait()
    state = start_v[...].astype(F32)
    waited = {"start"}

    def need(name):
        if name not in waited:
            waited.add(name)
            loads[name].wait()

    def gated(pre):
        sig = sigmoid(pre)
        return (pre * sig).astype(BF16), sig * (1.0 + pre * (1.0 - sig))

    err_parts = []
    for n in range(steps):
        h = columns[:, n : n + 1]
        keep = columns[:, steps + n : steps + n + 1]
        root = jnp.sqrt(h)
        low = state.astype(BF16)
        low_v[n * rows : (n + 1) * rows, :] = low
        need("spread")
        inner, slope = gated(mm(low, w_spread[...]))
        d_one[n] = slope
        need("scale")
        sig_g = sigmoid(mm(inner, w_scale[...]) + b_scale)
        spread = 0.6 * sig_g
        d_g[n] = spread * (1.0 - sig_g)
        shifted_low = (state + spread * root).astype(BF16)
        inner, slope = gated(mm(shifted_low, w_spread[...]))
        d_two[n] = slope
        sig_s = sigmoid(mm(inner, w_scale[...]) + b_scale)
        shifted = 0.6 * sig_s
        d_gbar[n] = shifted * (1.0 - sig_s)
        need("up")
        hidden, slope = gated(mm(low, w_up[...]) + b_up)
        hid_v[n * rows : (n + 1) * rows, :] = hidden
        d_pre[n] = slope
        need("noise")
        brownian = root * noise_v[n].astype(F32)
        factor = (brownian * brownian - h) / (2.0 * root)
        dw_v[n] = brownian
        fac_v[n] = factor
        milstein = (shifted - spread) * factor
        scaled = milstein / (abs_tol + rel_tol * jnp.abs(state))
        err_parts.append(jnp.sum((scaled * scaled).reshape(rows // 8, 8, latent), axis=0))
        if n + 1 < steps:
            need("down")
            drift = mm(hidden, w_down[...])
            proposal = state + drift * h + spread * brownian + milstein
            state = keep * proposal + (1.0 - keep) * state

    err_rows = [jnp.sum(jnp.sum(p, axis=0, keepdims=True), axis=1, keepdims=True) for p in err_parts]
    row = lax.broadcasted_iota(jnp.int32, err_ref.shape, 0)
    err = jnp.zeros(err_ref.shape, F32)
    for n in range(steps):
        err = jnp.where(row == n, err_rows[n], err)
    err_ref[...] = err

    need("down")
    need("cot")
    cot = cot_v[...].astype(F32)

    def through_net(d_out, slope):
        d_inner = mm_t(d_out.astype(BF16), w_scale[...]).astype(BF16).astype(F32)
        return mm_t((d_inner * slope).astype(BF16), w_spread[...]).astype(BF16).astype(F32)

    for n in reversed(range(steps)):
        h = columns[:, n : n + 1]
        keep = columns[:, steps + n : steps + n + 1]
        root = jnp.sqrt(h)
        kept = cot * keep
        cdrift = (kept * h).astype(BF16)
        cdrift_v[n * rows : (n + 1) * rows, :] = cdrift
        cpre = (mm_t(cdrift, w_down[...]) * d_pre[n]).astype(BF16)
        cpre_v[n * rows : (n + 1) * rows, :] = cpre
        if n > 0:
            d_shift = kept * fac_v[n]
            d_state = through_net(d_shift * d_gbar[n], d_two[n])
            d_spread = kept * dw_v[n] - d_shift + d_state * root
            d_first = through_net(d_spread * d_g[n], d_one[n])
            cot = (kept + (1.0 - keep) * cot) + d_state + d_first + mm_t(cpre, w_up[...])

    tiles = w_up.shape[1] // 128

    def place(grad, first):
        for block in range(latent // 8):
            core = block % 2
            at = (block // 2) % far
            up = block // (2 * far)
            for t in range(tiles):
                out_v[core, at, up, (first + t) * 8 : (first + t + 1) * 8, :] = grad[
                    block * 8 : (block + 1) * 8, t * 128 : (t + 1) * 128
                ]

    place(t_mm(cdrift_v[...], hid_v[...]), tiles)
    place(t_mm(low_v[...], cpre_v[...]), 0)
    own = core_ref[0]
    out = pltpu.make_async_copy(out_v.at[1 - own], send_hbm, out_sems.at[0])
    stay = pltpu.make_async_copy(out_v.at[own], keep_hbm, out_sems.at[1])
    out.start()
    stay.start()
    out.wait()
    stay.wait()


def run_steps(core, *args):
    start, w_up, _, _, _, _, _, noise, _, _, _ = args
    steps, rows, latent = noise.shape
    wide = w_up.shape[1]
    far = lax.axis_size("dp_1")
    near = lax.axis_size("dp_0")
    block = (far, near, 2 * wide // 16, 128)
    hbm = pl.BlockSpec(memory_space=pl.ANY)
    vmem = pl.BlockSpec(memory_space=pltpu.VMEM)
    smem = pl.BlockSpec(memory_space=pltpu.SMEM)
    half = jax.ShapeDtypeStruct((far, near, 2 * wide // 16, 128), F32)
    del block
    half = jax.ShapeDtypeStruct((far, near, wide // 8, 128), F32)
    return pl.pallas_call(
        steps_kernel,
        out_shape=(half, half, jax.ShapeDtypeStruct((8, 128), F32)),
        in_specs=[smem, hbm, hbm, vmem, hbm, hbm, hbm, vmem, hbm, vmem, vmem, hbm],
        out_specs=(hbm, hbm, vmem),
        scratch_shapes=[
            pltpu.VMEM((rows, latent), BF16),
            pltpu.VMEM((latent, wide), BF16),
            pltpu.VMEM((wide, latent), BF16),
            pltpu.VMEM((latent, wide), BF16),
            pltpu.VMEM((wide, latent), BF16),
            pltpu.VMEM((steps, rows, latent), BF16),
            pltpu.VMEM((rows, latent), BF16),
            pltpu.VMEM((steps, rows, wide), F32),
            pltpu.VMEM((steps, rows, wide), F32),
            pltpu.VMEM((steps, rows, wide), F32),
            pltpu.VMEM((steps * rows, wide), BF16),
            pltpu.VMEM((steps * rows, latent), BF16),
            pltpu.VMEM((steps * rows, wide), BF16),
            pltpu.VMEM((steps * rows, latent), BF16),
            pltpu.VMEM((steps, rows, latent), F32),
            pltpu.VMEM((steps, rows, latent), F32),
            pltpu.VMEM((steps, rows, latent), F32),
            pltpu.VMEM((steps, rows, latent), F32),
            pltpu.VMEM((2, far, near, wide // 8, 128), F32),
            pltpu.SemaphoreType.DMA((7,)),
            pltpu.SemaphoreType.DMA((2,)),
        ],
        compiler_params=pltpu.CompilerParams(vmem_limit_bytes=60 * 1024 * 1024),
        name="milstein_steps",
    )(core, *args)


def swap_sum(value, axis, distance):
    size = lax.axis_size(axis)
    pairs = [(k, (k + distance) % size) for k in range(size)]
    return value + lax.ppermute(value, axis, pairs)


def per_device(
    start_state, w_up, b_up, w_down, w_spread, w_scale, b_scale,
    brownian_noise, step_mults, accept_flags, cotangent,
):
    groups = lax.axis_size("grp")
    members = lax.axis_size(DP)
    far = lax.axis_size("dp_1")
    near = lax.axis_size("dp_0")
    row_count = start_state.shape[0] * start_state.shape[1] * groups * members
    wide = w_up.shape[1]
    core = lax.axis_index("dp_2")[None]
    keep, send, err = run_steps(
        core, start_state, w_up, b_up[None], w_down, w_spread, w_scale, b_scale[None],
        brownian_noise, step_mults, accept_flags, cotangent,
    )
    mine = keep + lax.ppermute(send, "dp_2", [(0, 1), (1, 0)])
    parts = lax.all_to_all(mine, "dp_1", 0, 0, tiled=True)
    column = jnp.sum(parts, axis=0)
    pieces = column.reshape(near * groups, -1, 128)
    arrived = lax.all_to_all(pieces, ("dp_0", "grp"), 0, 0, tiled=True)
    piece = jnp.sum(arrived, axis=0)
    copies = jnp.broadcast_to(piece, (groups, *piece.shape))
    whole = lax.all_to_all(copies, "grp", 0, 0, tiled=True)
    grads = whole.reshape(2, wide // 128, 8, 128).transpose(0, 2, 1, 3).reshape(2, 8, wide)

    for axis in ("dp_2", "dp_1", "dp_0", "grp"):
        distance = 1
        while distance < lax.axis_size(axis):
            err = swap_sum(err, axis, distance)
            distance *= 2
    err_norms = jnp.sqrt(err[: brownian_noise.shape[0], 0] / row_count)
    return (err_norms, grads[0], grads[1])


def solution(mesh):
    split = Mesh(mesh.devices.reshape(mesh.shape["grp"], 8, 4, 2), ("grp", "dp_0", "dp_1", "dp_2"))
    return jax.shard_map(
        per_device,
        mesh=split,
        in_specs=(
            P(GRP_DP, None), P(), P(), P(), P(), P(), P(),
            P(None, GRP_DP, None), P(None, GRP_DP), P(None, GRP_DP), P(GRP_DP, None),
        ),
        out_specs=(P(), P(DP, None), P(DP, None)),
        check_vma=False,
    )
```

```python
import jax
import jax.numpy as jnp
from jax import lax
from jax.experimental import pallas as pl
from jax.experimental.pallas import tpu as pltpu
from jax.sharding import Mesh
from jax.sharding import PartitionSpec as P

GRP = ("z_far", "z_mid", "z_pair")
DP = ("y_far", "y_pair", "x", "core")
GRP_DP = GRP + DP

base_step = 0.05
abs_tol = 0.01
rel_tol = 0.01
F32 = jnp.float32
BF16 = jnp.bfloat16
X = 4
PAIR = 2


def mm(a, b):
    return jnp.dot(a, b, preferred_element_type=F32)


def mm_t(a, b):
    return lax.dot_general(a, b, (((1,), (1,)), ((), ())), preferred_element_type=F32)


def t_mm(a, b):
    return lax.dot_general(a, b, (((0,), (0,)), ((), ())), preferred_element_type=F32)


def sigmoid(x):
    return 0.5 * jnp.tanh(0.5 * x) + 0.5


def steps_kernel(
    core_ref,
    start_hbm, w_up_hbm, b_up_hbm, w_down_hbm, w_spread_hbm, w_scale_hbm, b_scale_hbm,
    noise_hbm, mults_hbm, flags_hbm, cot_hbm,
    keep_ref, send_ref,
    start_v, w_up, b_up_v, w_down, w_spread, w_scale, b_scale_v, noise_v, mults_v, flags_v, cot_v,
    d_pre, d_one, d_two, hid_v, low_v, cpre_v, cdrift_v, d_g, d_gbar, fac_v, dw_v,
    in_sems,
):
    steps, rows, latent = noise_v.shape
    loads = {}
    for slot, (name, src, dst) in enumerate((
        ("start", start_hbm, start_v),
        ("mults", mults_hbm, mults_v),
        ("flags", flags_hbm, flags_v),
        ("b_up", b_up_hbm, b_up_v),
        ("b_scale", b_scale_hbm, b_scale_v),
        ("spread", w_spread_hbm, w_spread),
        ("scale", w_scale_hbm, w_scale),
        ("up", w_up_hbm, w_up),
        ("noise", noise_hbm, noise_v),
        ("down", w_down_hbm, w_down),
        ("cot", cot_hbm, cot_v),
    )):
        loads[name] = pltpu.make_async_copy(src, dst, in_sems.at[slot])
        loads[name].start()

    def need(*names):
        for name in names:
            if name in loads:
                loads.pop(name).wait()

    need("start", "mults", "flags", "b_up", "b_scale")
    per_row = jnp.concatenate(
        [
            mults_v[...].astype(F32) * base_step,
            flags_v[...].astype(F32),
            jnp.zeros((8 - 2 * steps, rows), F32),
        ],
        axis=0,
    )
    columns = jnp.transpose(per_row)
    b_up = b_up_v[...]
    b_scale = b_scale_v[...]
    state = start_v[...].astype(F32)

    def gated(pre):
        sig = sigmoid(pre)
        return (pre * sig).astype(BF16), sig * (1.0 + pre * (1.0 - sig))

    err_parts = []
    for n in range(steps):
        h = columns[:, n : n + 1]
        keep = columns[:, steps + n : steps + n + 1]
        root = jnp.sqrt(h)
        low = state.astype(BF16)
        low_v[n * rows : (n + 1) * rows, :] = low
        need("spread")
        inner, slope = gated(mm(low, w_spread[...]))
        d_one[n] = slope
        need("scale")
        sig_g = sigmoid(mm(inner, w_scale[...]) + b_scale)
        spread = 0.6 * sig_g
        d_g[n] = spread * (1.0 - sig_g)
        shifted_low = (state + spread * root).astype(BF16)
        inner, slope = gated(mm(shifted_low, w_spread[...]))
        d_two[n] = slope
        sig_s = sigmoid(mm(inner, w_scale[...]) + b_scale)
        shifted = 0.6 * sig_s
        d_gbar[n] = shifted * (1.0 - sig_s)
        need("up")
        hidden, slope = gated(mm(low, w_up[...]) + b_up)
        hid_v[n * rows : (n + 1) * rows, :] = hidden
        d_pre[n] = slope
        need("noise")
        brownian = root * noise_v[n].astype(F32)
        factor = (brownian * brownian - h) / (2.0 * root)
        dw_v[n] = brownian
        fac_v[n] = factor
        milstein = (shifted - spread) * factor
        scaled = milstein / (abs_tol + rel_tol * jnp.abs(state))
        err_parts.append(jnp.sum((scaled * scaled).reshape(rows // 8, 8, latent), axis=0))
        if n + 1 < steps:
            need("down")
            drift = mm(hidden, w_down[...])
            proposal = state + drift * h + spread * brownian + milstein
            state = keep * proposal + (1.0 - keep) * state

    err_rows = [jnp.sum(jnp.sum(p, axis=0, keepdims=True), axis=1, keepdims=True) for p in err_parts]
    row = lax.broadcasted_iota(jnp.int32, (8, 128), 0)
    err = jnp.zeros((8, 128), F32)
    for n in range(steps):
        err = jnp.where(row == n, err_rows[n], err)

    need("down")
    need("cot")
    cot = cot_v[...].astype(F32)

    def through_net(d_out, slope):
        d_inner = mm_t(d_out.astype(BF16), w_scale[...]).astype(BF16).astype(F32)
        return mm_t((d_inner * slope).astype(BF16), w_spread[...]).astype(BF16).astype(F32)

    for n in reversed(range(steps)):
        h = columns[:, n : n + 1]
        keep = columns[:, steps + n : steps + n + 1]
        root = jnp.sqrt(h)
        kept = cot * keep
        cdrift = (kept * h).astype(BF16)
        cdrift_v[n * rows : (n + 1) * rows, :] = cdrift
        cpre = (mm_t(cdrift, w_down[...]) * d_pre[n]).astype(BF16)
        cpre_v[n * rows : (n + 1) * rows, :] = cpre
        if n > 0:
            d_shift = kept * fac_v[n]
            d_state = through_net(d_shift * d_gbar[n], d_two[n])
            d_spread = kept * dw_v[n] - d_shift + d_state * root
            d_first = through_net(d_spread * d_g[n], d_one[n])
            cot = (kept + (1.0 - keep) * cot) + d_state + d_first + mm_t(cpre, w_up[...])

    tiles = w_up.shape[1] // 128
    sums = keep_ref.shape[1] - 8
    first = core_ref[0] == 0

    def place(grad, which):
        for q in range(latent // 16):
            far, pair, x = q // (PAIR * X), q // X % PAIR, q % X
            part = (x * PAIR + pair) * 2 + which
            for t in range(tiles):
                even = grad[16 * q : 16 * q + 8, t * 128 : (t + 1) * 128]
                odd = grad[16 * q + 8 : 16 * q + 16, t * 128 : (t + 1) * 128]
                at = (far * tiles + t) * 8
                keep_ref[part, at : at + 8, :] = jnp.where(first, even, odd)
                send_ref[part, at : at + 8, :] = jnp.where(first, odd, even)

    for part in range(keep_ref.shape[0]):
        keep_ref[part, sums : sums + 8, :] = err
        send_ref[part, sums : sums + 8, :] = err
    place(t_mm(cdrift_v[...], hid_v[...]), 1)
    place(t_mm(low_v[...], cpre_v[...]), 0)


def run_steps(core, *args):
    start, w_up, _, _, _, _, _, noise, _, _, _ = args
    steps, rows, latent = noise.shape
    wide = w_up.shape[1]
    parts = X * PAIR * 2
    hbm = pl.BlockSpec(memory_space=pltpu.HBM)
    vmem = pl.BlockSpec(memory_space=pltpu.VMEM)
    smem = pl.BlockSpec(memory_space=pltpu.SMEM)
    half = pltpu.VMEM((parts, latent * wide // (parts * 128) + 8, 128), F32)
    return pl.pallas_call(
        steps_kernel,
        out_shape=(half, half),
        in_specs=[smem] + [hbm] * len(args),
        out_specs=(vmem, vmem),
        scratch_shapes=[
            *(pltpu.VMEM(a.shape, a.dtype) for a in args),
            pltpu.VMEM((steps, rows, wide), F32),
            pltpu.VMEM((steps, rows, wide), F32),
            pltpu.VMEM((steps, rows, wide), F32),
            pltpu.VMEM((steps * rows, wide), BF16),
            pltpu.VMEM((steps * rows, latent), BF16),
            pltpu.VMEM((steps * rows, wide), BF16),
            pltpu.VMEM((steps * rows, latent), BF16),
            pltpu.VMEM((steps, rows, latent), F32),
            pltpu.VMEM((steps, rows, latent), F32),
            pltpu.VMEM((steps, rows, latent), F32),
            pltpu.VMEM((steps, rows, latent), F32),
            pltpu.SemaphoreType.DMA((len(args),)),
        ],
        compiler_params=pltpu.CompilerParams(vmem_limit_bytes=32 * 1024 * 1024),
        name="milstein_steps",
    )(core, *(pltpu.with_memory_space_constraint(a, pltpu.HBM) for a in args))


def summed(parts, axes):
    return jnp.sum(lax.all_to_all(parts, axes, 0, 0, tiled=True), axis=0)


def per_device(
    start_state, w_up, b_up, w_down, w_spread, w_scale, b_scale,
    brownian_noise, step_mults, accept_flags, cotangent,
):
    groups = lax.axis_size(GRP)
    members = lax.axis_size(DP)
    row_count = start_state.shape[0] * start_state.shape[1] * groups * members
    steps = brownian_noise.shape[0]
    wide = w_up.shape[1]
    core = lax.axis_index("core")[None]
    keep, send = run_steps(
        core, start_state, w_up, b_up[None], w_down, w_spread, w_scale, b_scale[None],
        brownian_noise, step_mults, accept_flags, cotangent,
    )
    mine = keep + lax.ppermute(send, "core", [(0, 1), (1, 0)])
    part = summed(mine, ("x", "y_pair", "z_pair"))
    far = lax.axis_size("y_far")
    sums, err = part[:-8].reshape(far, -1, 128), part[-8:]
    pieces = jnp.concatenate([sums, jnp.broadcast_to(err, (far, 8, 128))], axis=1)
    piece = summed(pieces, "y_far")
    copies = jnp.broadcast_to(piece, (groups, *piece.shape))
    arrived = lax.all_to_all(copies, GRP, 0, 0, tiled=True)
    whole = jnp.sum(arrived.reshape(groups // 2, 2, *piece.shape), axis=0)
    grads = whole[:, :-8].reshape(2, wide // 128, 8, 128).transpose(0, 2, 1, 3).reshape(2, 8, wide)
    err_norms = jnp.sqrt(whole[0, -8 : steps - 8, 0] / row_count)
    return (err_norms, grads[0], grads[1])


def solution(mesh):
    split = Mesh(mesh.devices.reshape(mesh.shape["grp"] // 4, 2, 2, -1, PAIR, X, 2), GRP_DP)
    return jax.shard_map(
        per_device,
        mesh=split,
        in_specs=(
            P(GRP_DP, None), P(), P(), P(), P(), P(), P(),
            P(None, GRP_DP, None), P(None, GRP_DP), P(None, GRP_DP), P(GRP_DP, None),
        ),
        out_specs=(P(), P(DP, None), P(DP, None)),
        check_vma=False,
    )
```

```python
import jax
import jax.numpy as jnp
from jax import lax
from jax.experimental import pallas as pl
from jax.experimental.pallas import tpu as pltpu
from jax.sharding import Mesh
from jax.sharding import PartitionSpec as P

GRP = ("z_far", "z_mid", "z_pair")
DP = ("y_far", "y_pair", "x", "core")
GRP_DP = GRP + DP

base_step = 0.05
abs_tol = 0.01
rel_tol = 0.01
F32 = jnp.float32
BF16 = jnp.bfloat16
X = 4
PAIR = 2


def mm(a, b):
    return jnp.dot(a, b, preferred_element_type=F32)


def mm_t(a, b):
    return lax.dot_general(a, b, (((1,), (1,)), ((), ())), preferred_element_type=F32)


def t_mm(a, b):
    return lax.dot_general(a, b, (((0,), (0,)), ((), ())), preferred_element_type=F32)


def sigmoid(x):
    return 0.5 * jnp.tanh(0.5 * x) + 0.5


def steps_kernel(
    core_ref,
    start_hbm, w_up_hbm, b_up_hbm, w_down_hbm, w_spread_hbm, w_scale_hbm, b_scale_hbm,
    noise_hbm, mults_hbm, flags_hbm, cot_hbm,
    keep_ref, send_ref,
    start_v, w_up, b_up_v, w_down, w_spread, w_scale, b_scale_v, noise_v, mults_v, flags_v, cot_v,
    d_pre, d_one, d_two, hid_v, low_v, cpre_v, cdrift_v, d_g, d_gbar, fac_v, dw_v,
    wt_down, wt_up, wt_scale, wt_spread,
    in_sems,
):
    steps, rows, latent = noise_v.shape
    loads = {}
    for slot, (name, src, dst) in enumerate((
        ("start", start_hbm, start_v),
        ("mults", mults_hbm, mults_v),
        ("flags", flags_hbm, flags_v),
        ("b_up", b_up_hbm, b_up_v),
        ("b_scale", b_scale_hbm, b_scale_v),
        ("spread", w_spread_hbm, w_spread),
        ("scale", w_scale_hbm, w_scale),
        ("up", w_up_hbm, w_up),
        ("noise", noise_hbm, noise_v),
        ("down", w_down_hbm, w_down),
        ("cot", cot_hbm, cot_v),
    )):
        loads[name] = pltpu.make_async_copy(src, dst, in_sems.at[slot])
        loads[name].start()

    def need(*names):
        for name in names:
            if name in loads:
                loads.pop(name).wait()

    need("start", "mults", "flags", "b_up", "b_scale")
    per_row = jnp.concatenate(
        [
            mults_v[...].astype(F32) * base_step,
            flags_v[...].astype(F32),
            jnp.zeros((8 - 2 * steps, rows), F32),
        ],
        axis=0,
    )
    columns = jnp.transpose(per_row)
    b_up = b_up_v[...]
    b_scale = b_scale_v[...]
    state = start_v[...].astype(F32)

    def gated(pre):
        sig = sigmoid(pre)
        return (pre * sig).astype(BF16), sig * (1.0 + pre * (1.0 - sig))

    err_parts = []
    for n in range(steps):
        h = columns[:, n : n + 1]
        keep = columns[:, steps + n : steps + n + 1]
        root = jnp.sqrt(h)
        low = state.astype(BF16)
        low_v[n * rows : (n + 1) * rows, :] = low
        need("spread")
        inner, slope = gated(mm(low, w_spread[...]))
        d_one[n] = slope
        need("scale")
        sig_g = sigmoid(mm(inner, w_scale[...]) + b_scale)
        spread = 0.6 * sig_g
        d_g[n] = spread * (1.0 - sig_g)
        shifted_low = (state + spread * root).astype(BF16)
        inner, slope = gated(mm(shifted_low, w_spread[...]))
        d_two[n] = slope
        sig_s = sigmoid(mm(inner, w_scale[...]) + b_scale)
        shifted = 0.6 * sig_s
        d_gbar[n] = shifted * (1.0 - sig_s)
        need("up")
        hidden, slope = gated(mm(low, w_up[...]) + b_up)
        hid_v[n * rows : (n + 1) * rows, :] = hidden
        d_pre[n] = slope
        need("noise")
        brownian = root * noise_v[n].astype(F32)
        factor = (brownian * brownian - h) / (2.0 * root)
        dw_v[n] = brownian
        fac_v[n] = factor
        milstein = (shifted - spread) * factor
        scaled = milstein / (abs_tol + rel_tol * jnp.abs(state))
        err_parts.append(jnp.sum((scaled * scaled).reshape(rows // 8, 8, latent), axis=0))
        if n + 1 < steps:
            need("down")
            drift = mm(hidden, w_down[...])
            proposal = state + drift * h + spread * brownian + milstein
            state = keep * proposal + (1.0 - keep) * state
            if n == 1:
                wt_down[...] = jnp.transpose(w_down[...])
                wt_scale[...] = jnp.transpose(w_scale[...])
                wt_spread[...] = jnp.transpose(w_spread[...])
                wt_up[...] = jnp.transpose(w_up[...])

    err_rows = [jnp.sum(jnp.sum(p, axis=0, keepdims=True), axis=1, keepdims=True) for p in err_parts]
    row = lax.broadcasted_iota(jnp.int32, (8, 128), 0)
    err = jnp.zeros((8, 128), F32)
    for n in range(steps):
        err = jnp.where(row == n, err_rows[n], err)

    need("down")
    need("cot")
    cot = cot_v[...].astype(F32)

    def through_net(d_out, slope):
        d_inner = mm(d_out.astype(BF16), wt_scale[...]).astype(BF16).astype(F32)
        return mm((d_inner * slope).astype(BF16), wt_spread[...]).astype(BF16).astype(F32)

    for n in reversed(range(steps)):
        h = columns[:, n : n + 1]
        keep = columns[:, steps + n : steps + n + 1]
        root = jnp.sqrt(h)
        kept = cot * keep
        cdrift = (kept * h).astype(BF16)
        cdrift_v[n * rows : (n + 1) * rows, :] = cdrift
        cpre = (mm(cdrift, wt_down[...]) * d_pre[n]).astype(BF16)
        cpre_v[n * rows : (n + 1) * rows, :] = cpre
        if n > 0:
            d_shift = kept * fac_v[n]
            d_state = through_net(d_shift * d_gbar[n], d_two[n])
            d_spread = kept * dw_v[n] - d_shift + d_state * root
            d_first = through_net(d_spread * d_g[n], d_one[n])
            cot = (kept + (1.0 - keep) * cot) + d_state + d_first + mm(cpre, wt_up[...])

    tiles = w_up.shape[1] // 128
    sums = keep_ref.shape[1] - 8
    first = core_ref[0] == 0

    def place(grad, which):
        for q in range(latent // 16):
            far, pair, x = q // (PAIR * X), q // X % PAIR, q % X
            part = (x * PAIR + pair) * 2 + which
            for t in range(tiles):
                even = grad[16 * q : 16 * q + 8, t * 128 : (t + 1) * 128]
                odd = grad[16 * q + 8 : 16 * q + 16, t * 128 : (t + 1) * 128]
                at = (far * tiles + t) * 8
                keep_ref[part, at : at + 8, :] = jnp.where(first, even, odd)
                send_ref[part, at : at + 8, :] = jnp.where(first, odd, even)

    for part in range(keep_ref.shape[0]):
        keep_ref[part, sums : sums + 8, :] = err
        send_ref[part, sums : sums + 8, :] = err
    place(t_mm(cdrift_v[...], hid_v[...]), 1)
    place(t_mm(low_v[...], cpre_v[...]), 0)


def run_steps(core, *args):
    start, w_up, _, _, _, _, _, noise, _, _, _ = args
    steps, rows, latent = noise.shape
    wide = w_up.shape[1]
    parts = X * PAIR * 2
    hbm = pl.BlockSpec(memory_space=pltpu.HBM)
    vmem = pl.BlockSpec(memory_space=pltpu.VMEM)
    smem = pl.BlockSpec(memory_space=pltpu.SMEM)
    half = pltpu.VMEM((parts, latent * wide // (parts * 128) + 8, 128), F32)
    return pl.pallas_call(
        steps_kernel,
        out_shape=(half, half),
        in_specs=[smem] + [hbm] * len(args),
        out_specs=(vmem, vmem),
        scratch_shapes=[
            *(pltpu.VMEM(a.shape, a.dtype) for a in args),
            pltpu.VMEM((steps, rows, wide), F32),
            pltpu.VMEM((steps, rows, wide), F32),
            pltpu.VMEM((steps, rows, wide), F32),
            pltpu.VMEM((steps * rows, wide), BF16),
            pltpu.VMEM((steps * rows, latent), BF16),
            pltpu.VMEM((steps * rows, wide), BF16),
            pltpu.VMEM((steps * rows, latent), BF16),
            pltpu.VMEM((steps, rows, latent), F32),
            pltpu.VMEM((steps, rows, latent), F32),
            pltpu.VMEM((steps, rows, latent), F32),
            pltpu.VMEM((steps, rows, latent), F32),
            pltpu.VMEM((latent, wide), BF16),
            pltpu.VMEM((wide, latent), BF16),
            pltpu.VMEM((latent, wide), BF16),
            pltpu.VMEM((wide, latent), BF16),
            pltpu.SemaphoreType.DMA((len(args),)),
        ],
        compiler_params=pltpu.CompilerParams(vmem_limit_bytes=32 * 1024 * 1024),
        name="milstein_steps",
    )(core, *(pltpu.with_memory_space_constraint(a, pltpu.HBM) for a in args))


def summed(parts, axes):
    return jnp.sum(lax.all_to_all(parts, axes, 0, 0, tiled=True), axis=0)


def per_device(
    start_state, w_up, b_up, w_down, w_spread, w_scale, b_scale,
    brownian_noise, step_mults, accept_flags, cotangent,
):
    groups = lax.axis_size(GRP)
    members = lax.axis_size(DP)
    row_count = start_state.shape[0] * start_state.shape[1] * groups * members
    steps = brownian_noise.shape[0]
    wide = w_up.shape[1]
    core = lax.axis_index("core")[None]
    keep, send = run_steps(
        core, start_state, w_up, b_up[None], w_down, w_spread, w_scale, b_scale[None],
        brownian_noise, step_mults, accept_flags, cotangent,
    )
    mine = keep + lax.ppermute(send, "core", [(0, 1), (1, 0)])
    part = summed(mine, ("x", "y_pair", "z_pair"))
    far = lax.axis_size("y_far")
    sums, err = part[:-8].reshape(far, -1, 128), part[-8:]
    pieces = jnp.concatenate([sums, jnp.broadcast_to(err, (far, 8, 128))], axis=1)
    piece = summed(pieces, "y_far")
    copies = jnp.broadcast_to(piece, (groups, *piece.shape))
    arrived = lax.all_to_all(copies, GRP, 0, 0, tiled=True)
    whole = jnp.sum(arrived.reshape(groups // 2, 2, *piece.shape), axis=0)
    grads = whole[:, :-8].reshape(2, wide // 128, 8, 128).transpose(0, 2, 1, 3).reshape(2, 8, wide)
    err_norms = jnp.sqrt(whole[0, -8 : steps - 8, 0] / row_count)
    return (err_norms, grads[0], grads[1])


def solution(mesh):
    split = Mesh(mesh.devices.reshape(mesh.shape["grp"] // 4, 2, 2, -1, PAIR, X, 2), GRP_DP)
    return jax.shard_map(
        per_device,
        mesh=split,
        in_specs=(
            P(GRP_DP, None), P(), P(), P(), P(), P(), P(),
            P(None, GRP_DP, None), P(None, GRP_DP), P(None, GRP_DP), P(GRP_DP, None),
        ),
        out_specs=(P(), P(DP, None), P(DP, None)),
        check_vma=False,
    )
```

```python
import jax
import jax.numpy as jnp
from jax import lax
from jax.experimental import pallas as pl
from jax.experimental.pallas import tpu as pltpu
from jax.sharding import Mesh
from jax.sharding import PartitionSpec as P

GRP = ("z_far", "z_mid", "z_pair")
DP = ("y_far", "y_pair", "x", "core")
GRP_DP = GRP + DP

base_step = 0.05
abs_tol = 0.01
rel_tol = 0.01
F32 = jnp.float32
BF16 = jnp.bfloat16
X = 4
PAIR = 2


def mm(a, b):
    return jnp.dot(a, b, preferred_element_type=F32)


def mm_t(a, b):
    return lax.dot_general(a, b, (((1,), (1,)), ((), ())), preferred_element_type=F32)


def t_mm(a, b):
    return lax.dot_general(a, b, (((0,), (0,)), ((), ())), preferred_element_type=F32)


def sigmoid(x):
    return 0.5 * jnp.tanh(0.5 * x) + 0.5


def steps_kernel(
    core_ref,
    start_hbm, w_up_hbm, b_up_hbm, w_down_hbm, w_spread_hbm, w_scale_hbm, b_scale_hbm,
    noise_hbm, mults_hbm, flags_hbm, cot_hbm,
    keep_ref, send_ref,
    start_v, w_up, b_up_v, w_down, w_spread, w_scale, b_scale_v, noise_v, mults_v, flags_v, cot_v,
    d_pre, d_one, d_two, hid_v, low_v, cpre_v, cdrift_v, d_g, d_gbar, fac_v, dw_v,
    wt_down, wt_up, wt_scale, wt_spread,
    in_sems,
):
    steps, rows, latent = noise_v.shape
    loads = {}
    for slot, (name, src, dst) in enumerate((
        ("start", start_hbm, start_v),
        ("mults", mults_hbm, mults_v),
        ("flags", flags_hbm, flags_v),
        ("b_up", b_up_hbm, b_up_v),
        ("b_scale", b_scale_hbm, b_scale_v),
        ("spread", w_spread_hbm, w_spread),
        ("scale", w_scale_hbm, w_scale),
        ("up", w_up_hbm, w_up),
        ("noise", noise_hbm, noise_v),
        ("down", w_down_hbm, w_down),
        ("cot", cot_hbm, cot_v),
    )):
        loads[name] = pltpu.make_async_copy(src, dst, in_sems.at[slot])
        loads[name].start()

    def need(*names):
        for name in names:
            if name in loads:
                loads.pop(name).wait()

    need("start", "mults", "flags", "b_up", "b_scale")
    per_row = jnp.concatenate(
        [
            mults_v[...].astype(F32) * base_step,
            flags_v[...].astype(F32),
            jnp.zeros((8 - 2 * steps, rows), F32),
        ],
        axis=0,
    )
    columns = jnp.transpose(per_row)
    b_up = b_up_v[...]
    b_scale = b_scale_v[...]
    state = start_v[...].astype(F32)

    def gated(pre):
        sig = sigmoid(pre)
        return (pre * sig).astype(BF16), sig * (1.0 + pre * (1.0 - sig))

    err_parts = []
    for n in range(steps):
        h = columns[:, n : n + 1]
        keep = columns[:, steps + n : steps + n + 1]
        root = jnp.sqrt(h)
        low = state.astype(BF16)
        low_v[n * rows : (n + 1) * rows, :] = low
        need("spread")
        inner, slope = gated(mm(low, w_spread[...]))
        d_one[n] = slope
        need("scale")
        sig_g = sigmoid(mm(inner, w_scale[...]) + b_scale)
        spread = 0.6 * sig_g
        d_g[n] = spread * (1.0 - sig_g)
        shifted_low = (state + spread * root).astype(BF16)
        inner, slope = gated(mm(shifted_low, w_spread[...]))
        d_two[n] = slope
        sig_s = sigmoid(mm(inner, w_scale[...]) + b_scale)
        shifted = 0.6 * sig_s
        d_gbar[n] = shifted * (1.0 - sig_s)
        need("up", "noise", "down", "cot")
        hidden, slope = gated(mm(low, w_up[...]) + b_up)
        hid_v[n * rows : (n + 1) * rows, :] = hidden
        d_pre[n] = slope
        need("noise")
        brownian = root * noise_v[n].astype(F32)
        factor = (brownian * brownian - h) / (2.0 * root)
        dw_v[n] = brownian
        fac_v[n] = factor
        milstein = (shifted - spread) * factor
        scaled = milstein / (abs_tol + rel_tol * jnp.abs(state))
        err_parts.append(jnp.sum((scaled * scaled).reshape(rows // 8, 8, latent), axis=0))
        if n + 1 < steps:
            need("down")
            drift = mm(hidden, w_down[...])
            proposal = state + drift * h + spread * brownian + milstein
            state = keep * proposal + (1.0 - keep) * state
            if n == 1:
                wt_down[...] = jnp.transpose(w_down[...])
                wt_scale[...] = jnp.transpose(w_scale[...])
                wt_spread[...] = jnp.transpose(w_spread[...])
                wt_up[...] = jnp.transpose(w_up[...])

    err_rows = [jnp.sum(jnp.sum(p, axis=0, keepdims=True), axis=1, keepdims=True) for p in err_parts]
    row = lax.broadcasted_iota(jnp.int32, (8, 128), 0)
    err = jnp.zeros((8, 128), F32)
    for n in range(steps):
        err = jnp.where(row == n, err_rows[n], err)

    need("down")
    need("cot")
    cot = cot_v[...].astype(F32)

    def through_net(d_out, slope):
        d_inner = mm(d_out.astype(BF16), wt_scale[...]).astype(BF16).astype(F32)
        return mm((d_inner * slope).astype(BF16), wt_spread[...]).astype(BF16).astype(F32)

    for n in reversed(range(steps)):
        h = columns[:, n : n + 1]
        keep = columns[:, steps + n : steps + n + 1]
        root = jnp.sqrt(h)
        kept = cot * keep
        cdrift = (kept * h).astype(BF16)
        cdrift_v[n * rows : (n + 1) * rows, :] = cdrift
        cpre = (mm(cdrift, wt_down[...]) * d_pre[n]).astype(BF16)
        cpre_v[n * rows : (n + 1) * rows, :] = cpre
        if n > 0:
            d_shift = kept * fac_v[n]
            d_state = through_net(d_shift * d_gbar[n], d_two[n])
            d_spread = kept * dw_v[n] - d_shift + d_state * root
            d_first = through_net(d_spread * d_g[n], d_one[n])
            cot = (kept + (1.0 - keep) * cot) + d_state + d_first + mm(cpre, wt_up[...])

    tiles = w_up.shape[1] // 128
    sums = keep_ref.shape[1] - 8
    first = core_ref[0] == 0

    def place(grad, which):
        for q in range(latent // 16):
            far, pair, x = q // (PAIR * X), q // X % PAIR, q % X
            part = (x * PAIR + pair) * 2 + which
            for t in range(tiles):
                even = grad[16 * q : 16 * q + 8, t * 128 : (t + 1) * 128]
                odd = grad[16 * q + 8 : 16 * q + 16, t * 128 : (t + 1) * 128]
                at = (far * tiles + t) * 8
                keep_ref[part, at : at + 8, :] = jnp.where(first, even, odd)
                send_ref[part, at : at + 8, :] = jnp.where(first, odd, even)

    for part in range(keep_ref.shape[0]):
        keep_ref[part, sums : sums + 8, :] = err
        send_ref[part, sums : sums + 8, :] = err
    place(t_mm(cdrift_v[...], hid_v[...]), 1)
    place(t_mm(low_v[...], cpre_v[...]), 0)


def run_steps(core, *args):
    start, w_up, _, _, _, _, _, noise, _, _, _ = args
    steps, rows, latent = noise.shape
    wide = w_up.shape[1]
    parts = X * PAIR * 2
    hbm = pl.BlockSpec(memory_space=pltpu.HBM)
    vmem = pl.BlockSpec(memory_space=pltpu.VMEM)
    smem = pl.BlockSpec(memory_space=pltpu.SMEM)
    half = pltpu.VMEM((parts, latent * wide // (parts * 128) + 8, 128), F32)
    return pl.pallas_call(
        steps_kernel,
        out_shape=(half, half),
        in_specs=[smem] + [hbm] * len(args),
        out_specs=(vmem, vmem),
        scratch_shapes=[
            *(pltpu.VMEM(a.shape, a.dtype) for a in args),
            pltpu.VMEM((steps, rows, wide), F32),
            pltpu.VMEM((steps, rows, wide), F32),
            pltpu.VMEM((steps, rows, wide), F32),
            pltpu.VMEM((steps * rows, wide), BF16),
            pltpu.VMEM((steps * rows, latent), BF16),
            pltpu.VMEM((steps * rows, wide), BF16),
            pltpu.VMEM((steps * rows, latent), BF16),
            pltpu.VMEM((steps, rows, latent), F32),
            pltpu.VMEM((steps, rows, latent), F32),
            pltpu.VMEM((steps, rows, latent), F32),
            pltpu.VMEM((steps, rows, latent), F32),
            pltpu.VMEM((latent, wide), BF16),
            pltpu.VMEM((wide, latent), BF16),
            pltpu.VMEM((latent, wide), BF16),
            pltpu.VMEM((wide, latent), BF16),
            pltpu.SemaphoreType.DMA((len(args),)),
        ],
        compiler_params=pltpu.CompilerParams(vmem_limit_bytes=32 * 1024 * 1024),
        name="milstein_steps",
    )(core, *(pltpu.with_memory_space_constraint(a, pltpu.HBM) for a in args))


def finish(arrived, steps, wide, row_count):
    tiles = wide // 128
    sums = tiles * 8

    def kernel(arrived_ref, err_ref, up_ref, down_ref):
        def total(which, start, size):
            pieces = [arrived_ref[k, start : start + size, :] for k in range(which, arrived_ref.shape[0], 2)]
            while len(pieces) > 1:
                pieces = [a + b for a, b in zip(pieces[::2], pieces[1::2])]
            return pieces[0]

        for which, out in ((0, up_ref), (1, down_ref)):
            for t in range(tiles):
                out[:, t * 128 : (t + 1) * 128] = total(which, t * 8, 8)
        err = total(0, sums, 8)
        row = lax.broadcasted_iota(jnp.int32, err.shape, 0)
        lane = lax.broadcasted_iota(jnp.int32, err.shape, 1)
        norms = jnp.sqrt(jnp.sum(jnp.where(row == lane, err, 0.0), axis=0) / row_count)
        err_ref[...] = norms[:steps]

    vmem = pl.BlockSpec(memory_space=pltpu.VMEM)
    grad = jax.ShapeDtypeStruct((8, wide), F32)
    return pl.pallas_call(
        kernel,
        out_shape=(jax.ShapeDtypeStruct((steps,), F32), grad, grad),
        in_specs=[vmem],
        out_specs=(vmem, vmem, vmem),
        compiler_params=pltpu.CompilerParams(vmem_limit_bytes=4 * 1024 * 1024),
        name="finish",
    )(arrived)


def summed(parts, axes):
    return jnp.sum(lax.all_to_all(parts, axes, 0, 0, tiled=True), axis=0)


def per_device(
    start_state, w_up, b_up, w_down, w_spread, w_scale, b_scale,
    brownian_noise, step_mults, accept_flags, cotangent,
):
    groups = lax.axis_size(GRP)
    members = lax.axis_size(DP)
    row_count = start_state.shape[0] * start_state.shape[1] * groups * members
    steps = brownian_noise.shape[0]
    wide = w_up.shape[1]
    core = lax.axis_index("core")[None]
    keep, send = run_steps(
        core, start_state, w_up, b_up[None], w_down, w_spread, w_scale, b_scale[None],
        brownian_noise, step_mults, accept_flags, cotangent,
    )
    mine = keep + lax.ppermute(send, "core", [(0, 1), (1, 0)])
    part = summed(mine, ("x", "y_pair", "z_pair"))
    far = lax.axis_size("y_far")
    sums, err = part[:-8].reshape(far, -1, 128), part[-8:]
    pieces = jnp.concatenate([sums, jnp.broadcast_to(err, (far, 8, 128))], axis=1)
    piece = summed(pieces, "y_far")
    copies = jnp.broadcast_to(piece, (groups, *piece.shape))
    arrived = lax.all_to_all(copies, GRP, 0, 0, tiled=True)
    return finish(arrived, steps, wide, row_count)


def solution(mesh):
    split = Mesh(mesh.devices.reshape(mesh.shape["grp"] // 4, 2, 2, -1, PAIR, X, 2), GRP_DP)
    return jax.shard_map(
        per_device,
        mesh=split,
        in_specs=(
            P(GRP_DP, None), P(), P(), P(), P(), P(), P(),
            P(None, GRP_DP, None), P(None, GRP_DP), P(None, GRP_DP), P(GRP_DP, None),
        ),
        out_specs=(P(), P(DP, None), P(DP, None)),
        check_vma=False,
    )
```

```python
import jax
import jax.numpy as jnp
from jax import lax
from jax.experimental import pallas as pl
from jax.experimental.pallas import tpu as pltpu
from jax.sharding import Mesh
from jax.sharding import PartitionSpec as P

GRP = ("z_far", "z_mid", "z_pair")
DP = ("y_far", "y_pair", "x", "core")
GRP_DP = GRP + DP

base_step = 0.05
abs_tol = 0.01
rel_tol = 0.01
F32 = jnp.float32
BF16 = jnp.bfloat16
X = 4
PAIR = 2


def mm(a, b):
    return jnp.dot(a, b, preferred_element_type=F32)


def mm_t(a, b):
    return lax.dot_general(a, b, (((1,), (1,)), ((), ())), preferred_element_type=F32)


def t_mm(a, b):
    return lax.dot_general(a, b, (((0,), (0,)), ((), ())), preferred_element_type=F32)


def sigmoid(x):
    return 0.5 * jnp.tanh(0.5 * x) + 0.5


def steps_kernel(
    core_ref,
    start_hbm, w_up_hbm, b_up_hbm, w_down_hbm, w_spread_hbm, w_scale_hbm, b_scale_hbm,
    noise_hbm, mults_hbm, flags_hbm, cot_hbm,
    keep_ref, send_ref,
    start_v, w_up, b_up_v, w_down, w_spread, w_scale, b_scale_v, noise_v, mults_v, flags_v, cot_v,
    d_pre, d_one, d_two, hid_v, low_v, cpre_v, cdrift_v, d_g, d_gbar, fac_v, dw_v,
    wt_down, wt_up, wt_scale, wt_spread,
    in_sems,
):
    steps, rows, latent = noise_v.shape
    loads = {}
    for slot, (name, src, dst) in enumerate((
        ("start", start_hbm, start_v),
        ("mults", mults_hbm, mults_v),
        ("flags", flags_hbm, flags_v),
        ("b_up", b_up_hbm, b_up_v),
        ("b_scale", b_scale_hbm, b_scale_v),
        ("spread", w_spread_hbm, w_spread),
        ("scale", w_scale_hbm, w_scale),
        ("up", w_up_hbm, w_up),
        ("noise", noise_hbm, noise_v),
        ("down", w_down_hbm, w_down),
        ("cot", cot_hbm, cot_v),
    )):
        loads[name] = pltpu.make_async_copy(src, dst, in_sems.at[slot])
        loads[name].start()

    def need(*names):
        for name in names:
            if name in loads:
                loads.pop(name).wait()

    need("start", "mults", "flags", "b_up", "b_scale")
    per_row = jnp.concatenate(
        [
            mults_v[...].astype(F32) * base_step,
            flags_v[...].astype(F32),
            jnp.zeros((8 - 2 * steps, rows), F32),
        ],
        axis=0,
    )
    columns = jnp.transpose(per_row)
    b_up = b_up_v[...]
    b_scale = b_scale_v[...]
    state = start_v[...].astype(F32)

    def gated(pre):
        sig = sigmoid(pre)
        return (pre * sig).astype(BF16), sig * (1.0 + pre * (1.0 - sig))

    err_parts = []
    for n in range(steps):
        h = columns[:, n : n + 1]
        keep = columns[:, steps + n : steps + n + 1]
        root = jnp.sqrt(h)
        low = state.astype(BF16)
        low_v[n * rows : (n + 1) * rows, :] = low
        need("spread")
        inner, slope = gated(mm(low, w_spread[...]))
        d_one[n] = slope
        need("scale")
        sig_g = sigmoid(mm(inner, w_scale[...]) + b_scale)
        spread = 0.6 * sig_g
        d_g[n] = spread * (1.0 - sig_g)
        shifted_low = (state + spread * root).astype(BF16)
        inner, slope = gated(mm(shifted_low, w_spread[...]))
        d_two[n] = slope
        sig_s = sigmoid(mm(inner, w_scale[...]) + b_scale)
        shifted = 0.6 * sig_s
        d_gbar[n] = shifted * (1.0 - sig_s)
        need("up", "noise", "down", "cot")
        hidden, slope = gated(mm(low, w_up[...]) + b_up)
        hid_v[n * rows : (n + 1) * rows, :] = hidden
        d_pre[n] = slope
        need("noise")
        brownian = root * noise_v[n].astype(F32)
        factor = (brownian * brownian - h) / (2.0 * root)
        dw_v[n] = brownian
        fac_v[n] = factor
        milstein = (shifted - spread) * factor
        scaled = milstein / (abs_tol + rel_tol * jnp.abs(state))
        err_parts.append(jnp.sum((scaled * scaled).reshape(rows // 8, 8, latent), axis=0))
        if n + 1 < steps:
            need("down")
            drift = mm(hidden, w_down[...])
            proposal = state + drift * h + spread * brownian + milstein
            state = keep * proposal + (1.0 - keep) * state
            if n == 1:
                wt_down[...] = jnp.transpose(w_down[...])
                wt_scale[...] = jnp.transpose(w_scale[...])
                wt_spread[...] = jnp.transpose(w_spread[...])
                wt_up[...] = jnp.transpose(w_up[...])

    err_rows = [jnp.sum(jnp.sum(p, axis=0, keepdims=True), axis=1, keepdims=True) for p in err_parts]
    row = lax.broadcasted_iota(jnp.int32, (8, 128), 0)
    err = jnp.zeros((8, 128), F32)
    for n in range(steps):
        err = jnp.where(row == n, err_rows[n], err)

    need("down")
    need("cot")
    cot = cot_v[...].astype(F32)

    def through_net(d_out, slope):
        d_inner = mm(d_out.astype(BF16), wt_scale[...]).astype(BF16).astype(F32)
        return mm((d_inner * slope).astype(BF16), wt_spread[...]).astype(BF16).astype(F32)

    for n in reversed(range(steps)):
        h = columns[:, n : n + 1]
        keep = columns[:, steps + n : steps + n + 1]
        root = jnp.sqrt(h)
        kept = cot * keep
        cdrift = (kept * h).astype(BF16)
        cdrift_v[n * rows : (n + 1) * rows, :] = cdrift
        cpre = (mm(cdrift, wt_down[...]) * d_pre[n]).astype(BF16)
        cpre_v[n * rows : (n + 1) * rows, :] = cpre
        if n > 0:
            d_shift = kept * fac_v[n]
            d_state = through_net(d_shift * d_gbar[n], d_two[n])
            d_spread = kept * dw_v[n] - d_shift + d_state * root
            d_first = through_net(d_spread * d_g[n], d_one[n])
            cot = (kept + (1.0 - keep) * cot) + d_state + d_first + mm(cpre, wt_up[...])

    tiles = w_up.shape[1] // 128
    sums = keep_ref.shape[1] - 8
    first = core_ref[0] == 0

    def place(grad, which):
        for q in range(latent // 16):
            far, pair, x = q // (PAIR * X), q // X % PAIR, q % X
            part = (which * PAIR + pair) * X + x
            for t in range(tiles):
                even = grad[16 * q : 16 * q + 8, t * 128 : (t + 1) * 128]
                odd = grad[16 * q + 8 : 16 * q + 16, t * 128 : (t + 1) * 128]
                at = (far * tiles + t) * 8
                keep_ref[part, at : at + 8, :] = jnp.where(first, even, odd)
                send_ref[part, at : at + 8, :] = jnp.where(first, odd, even)

    for part in range(keep_ref.shape[0]):
        keep_ref[part, sums : sums + 8, :] = err
        send_ref[part, sums : sums + 8, :] = err
    place(t_mm(cdrift_v[...], hid_v[...]), 1)
    place(t_mm(low_v[...], cpre_v[...]), 0)


def run_steps(core, *args):
    start, w_up, _, _, _, _, _, noise, _, _, _ = args
    steps, rows, latent = noise.shape
    wide = w_up.shape[1]
    parts = X * PAIR * 2
    hbm = pl.BlockSpec(memory_space=pltpu.HBM)
    vmem = pl.BlockSpec(memory_space=pltpu.VMEM)
    smem = pl.BlockSpec(memory_space=pltpu.SMEM)
    half = pltpu.VMEM((parts, latent * wide // (parts * 128) + 8, 128), F32)
    return pl.pallas_call(
        steps_kernel,
        out_shape=(half, half),
        in_specs=[smem] + [hbm] * len(args),
        out_specs=(vmem, vmem),
        scratch_shapes=[
            *(pltpu.VMEM(a.shape, a.dtype) for a in args),
            pltpu.VMEM((steps, rows, wide), F32),
            pltpu.VMEM((steps, rows, wide), F32),
            pltpu.VMEM((steps, rows, wide), F32),
            pltpu.VMEM((steps * rows, wide), BF16),
            pltpu.VMEM((steps * rows, latent), BF16),
            pltpu.VMEM((steps * rows, wide), BF16),
            pltpu.VMEM((steps * rows, latent), BF16),
            pltpu.VMEM((steps, rows, latent), F32),
            pltpu.VMEM((steps, rows, latent), F32),
            pltpu.VMEM((steps, rows, latent), F32),
            pltpu.VMEM((steps, rows, latent), F32),
            pltpu.VMEM((latent, wide), BF16),
            pltpu.VMEM((wide, latent), BF16),
            pltpu.VMEM((latent, wide), BF16),
            pltpu.VMEM((wide, latent), BF16),
            pltpu.SemaphoreType.DMA((len(args),)),
        ],
        compiler_params=pltpu.CompilerParams(
            vmem_limit_bytes=32 * 1024 * 1024),
        name="milstein_steps",
    )(core, *(pltpu.with_memory_space_constraint(a, pltpu.HBM) for a in args))


def finish(arrived, steps, wide, row_count):
    tiles = wide // 128
    sums = tiles * 8

    def kernel(arrived_ref, err_ref, up_ref, down_ref):
        def total(which, start, size):
            pieces = [arrived_ref[k, start : start + size, :] for k in range(which, arrived_ref.shape[0], 2)]
            while len(pieces) > 1:
                pieces = [a + b for a, b in zip(pieces[::2], pieces[1::2])]
            return pieces[0]

        for which, out in ((0, up_ref), (1, down_ref)):
            for t in range(tiles):
                out[:, t * 128 : (t + 1) * 128] = total(which, t * 8, 8)
        err = total(0, sums, 8)
        row = lax.broadcasted_iota(jnp.int32, err.shape, 0)
        lane = lax.broadcasted_iota(jnp.int32, err.shape, 1)
        norms = jnp.sqrt(jnp.sum(jnp.where(row == lane, err, 0.0), axis=0) / row_count)
        err_ref[...] = norms[:steps]

    vmem = pl.BlockSpec(memory_space=pltpu.VMEM)
    grad = jax.ShapeDtypeStruct((8, wide), F32)
    return pl.pallas_call(
        kernel,
        out_shape=(jax.ShapeDtypeStruct((steps,), F32), grad, grad),
        in_specs=[vmem],
        out_specs=(vmem, vmem, vmem),
        compiler_params=pltpu.CompilerParams(vmem_limit_bytes=4 * 1024 * 1024),
        name="finish",
    )(arrived)


def summed(parts, axes):
    return jnp.sum(lax.all_to_all(parts, axes, 0, 0, tiled=True), axis=0)


def per_device(
    start_state, w_up, b_up, w_down, w_spread, w_scale, b_scale,
    brownian_noise, step_mults, accept_flags, cotangent,
):
    groups = lax.axis_size(GRP)
    members = lax.axis_size(DP)
    row_count = start_state.shape[0] * start_state.shape[1] * groups * members
    steps = brownian_noise.shape[0]
    wide = w_up.shape[1]
    core = lax.axis_index("core")[None]
    keep, send = run_steps(
        core, start_state, w_up, b_up[None], w_down, w_spread, w_scale, b_scale[None],
        brownian_noise, step_mults, accept_flags, cotangent,
    )
    mine = keep + lax.ppermute(send, "core", [(0, 1), (1, 0)])
    part = summed(mine, ("z_pair", "y_pair", "x"))
    far = lax.axis_size("y_far")
    sums, err = part[:-8].reshape(far, -1, 128), part[-8:]
    pieces = jnp.concatenate([sums, jnp.broadcast_to(err, (far, 8, 128))], axis=1)
    piece = summed(pieces, "y_far")
    copies = jnp.broadcast_to(piece, (groups, *piece.shape))
    arrived = lax.all_to_all(copies, GRP, 0, 0, tiled=True)
    return finish(arrived, steps, wide, row_count)


def solution(mesh):
    split = Mesh(mesh.devices.reshape(mesh.shape["grp"] // 4, 2, 2, -1, PAIR, X, 2), GRP_DP)
    return jax.shard_map(
        per_device,
        mesh=split,
        in_specs=(
            P(GRP_DP, None), P(), P(), P(), P(), P(), P(),
            P(None, GRP_DP, None), P(None, GRP_DP), P(None, GRP_DP), P(GRP_DP, None),
        ),
        out_specs=(P(), P(DP, None), P(DP, None)),
        check_vma=False,
    )
```
